32 devices in a mesh: tab: 2 (over x), cand: 4 (over z), dp: 4 (over y, core).
Axes of the slice: x: 2, y: 2, z: 4, core: 2. Of those that a mesh axis runs over, the one named last changes fastest.
Arguments:
- tables: bfloat16 [16, 65536, 128], P(('cand', 'dp'), 'tab'), may hold values from -6 to 6
- bag_ids: int32 [16, 1024, 16], P(('cand', 'dp')), may hold values from 0 to 65535
- bag_lengths: int32 [16, 1024], P(('cand', 'dp')), may hold values from 1 to 16
- item_weight: bfloat16 [2048, 256], replicated, may hold values from -0.125 to 0.125
- user_features: bfloat16 [16384, 512], P(('tab', 'dp')), may hold values from -6 to 6
- user_w1: bfloat16 [512, 1024], replicated, may hold values from -0.25 to 0.25
- user_w2: bfloat16 [1024, 256], replicated, may hold values from -0.1875 to 0.1875
- positive_items: int32 [16384], P(('tab', 'dp')), may hold values from 0 to 1023
Outputs:
- item_emb: float32 [1024, 256], P(('tab', 'cand', 'dp'))
- user_loss: float32 [16384], P(('tab', 'dp'))
The draws below stay inside these ranges and needn't reach their ends.
Inputs may be any that keep to these rules, and one draw needn't show every extreme that they name: `bag_ids`: row ids of a table. Only the first bag_lengths ids of a bag count; the rest is padding.
All inputs are finite; a program needn't handle non-finite values.
Results may differ from the reference program's by a relative error of at most 0.00046.
Values sent between devices are 32-bit elements; how exact they have to be, the bound alone decides.
No kernel may reach another device: no remote copies, remote signals or barrier semaphores. Data moves between devices by JAX's collectives and lax.ppermute only.
A program may use at most 64 MiB of HBM per device.

```python
import jax
import jax.numpy as jnp
from jax import lax

E = 128
H = 256
DU = 512
HU = 1024
L = 16
ITEMS = 1024
F = 16
VOCAB = 65536
USERS = 16384


def place_ends(array, stream_key, least, top_value):
    place = [jax.random.randint(jax.random.fold_in(stream_key, axis), (), 0, length) for axis, length in enumerate(array.shape)]
    main_axis = array.shape.index(max(array.shape))
    next_to = place[:main_axis] + [(place[main_axis] + 1) % array.shape[main_axis]] + place[main_axis + 1:]
    return array.at[tuple(place)].set(least).at[tuple(next_to)].set(top_value)


def levels(own_key, shape, pieces, least, largest):
    factor_of, own = 1.0, jax.random.fold_in(own_key, 6)
    for position, parts in pieces:
        heights = jnp.exp(jax.random.uniform(jax.random.fold_in(own, position), (parts,), jnp.float32, least / len(pieces), largest / len(pieces)))
        factor_of = factor_of * jnp.repeat(heights, shape[position] // parts).reshape([-1 if axis == position else 1 for axis in range(len(shape))])
    return factor_of


def noise(stream_key, extent, spread, limit, split=(), held_as=jnp.bfloat16):
    gain = levels(stream_key, extent, split, -0.22, 0.18) if split else 1.0
    result = jax.random.normal(stream_key, extent, jnp.float32) * spread * gain
    return jnp.minimum(jnp.maximum(result, -limit), limit).astype(held_as)


def setup_inputs(seed: int = 0) -> dict:
    splits = jax.random.split(jax.random.key(seed), 9)
    return {
        "tables": noise(splits[0], (F, VOCAB, E), 1.0, 6.0, ((0, 16), (1, 2))),
        "bag_ids": place_ends(jax.random.randint(splits[1], (F, ITEMS, L), 0, VOCAB), jax.random.fold_in(splits[1], 1), 0, VOCAB - 1).astype(jnp.int32),
        "bag_lengths": place_ends(jax.random.randint(splits[2], (F, ITEMS), 1, L + 1), jax.random.fold_in(splits[2], 1), 1, L).astype(jnp.int32),
        "item_weight": noise(splits[3], (F * E, H), (F * E) ** -0.5, 0.125),
        "user_features": noise(splits[4], (USERS, DU), 1.0, 6.0, ((0, 8),)),
        "user_w1": noise(splits[5], (DU, HU), DU ** -0.5, 0.25),
        "user_w2": noise(splits[6], (HU, H), HU ** -0.5, 0.1875),
        "positive_items": place_ends(jax.random.randint(splits[7], (USERS,), 0, ITEMS), jax.random.fold_in(splits[7], 1), 0, ITEMS - 1).astype(jnp.int32),
    }


epsilon = 1e-06
logit_scale = 20.0

def unit_rows(vectors):
    return vectors * lax.rsqrt(lax.optimization_barrier(jnp.mean(vectors * vectors, axis=-1, keepdims=True)) + epsilon)

def pool_table(inputs):
    table, bag_ids, lengths = inputs
    gathered = jnp.take(table, bag_ids, axis=0).astype(jnp.float32)
    valid = lax.broadcasted_iota(jnp.int32, bag_ids.shape, 1) < lengths[:, None]
    summed = lax.optimization_barrier(jnp.sum(jnp.where(valid[:, :, None], gathered, jnp.float32(0.0)), axis=1))
    return summed / lengths[:, None].astype(jnp.float32)

def reference(tables, bag_ids, bag_lengths, item_weight, user_features, user_w1, user_w2, positive_items):
    pooled = lax.map(pool_table, (tables, bag_ids, bag_lengths))
    joined = jnp.transpose(pooled, (1, 0, 2)).reshape(ITEMS, F * E)
    item_pre = jnp.dot(joined, item_weight.astype(jnp.float32), precision=lax.Precision.HIGHEST, preferred_element_type=jnp.float32)
    item_emb = unit_rows(item_pre)
    user_hidden = jax.nn.gelu(jnp.dot(user_features, user_w1, preferred_element_type=jnp.float32), approximate=False).astype(jnp.bfloat16)
    user_pre = jnp.dot(user_hidden, user_w2, preferred_element_type=jnp.float32)
    user_emb = unit_rows(user_pre)
    scores = jnp.dot(user_emb, item_emb.T, precision=lax.Precision.HIGHEST, preferred_element_type=jnp.float32) * (logit_scale / H)
    totals = lax.optimization_barrier(jnp.sum(jnp.exp(scores), axis=1))
    positive = jnp.take_along_axis(scores, positive_items[:, None].astype(jnp.int32), axis=1)[:, 0]
    user_loss = jnp.log(totals) - positive
    return (item_emb, user_loss)
```

```python
import functools

import jax
import jax.numpy as jnp
from jax import lax
from jax.experimental import pallas as pl
from jax.experimental.pallas import tpu as pltpu
from jax.sharding import PartitionSpec as P

epsilon = 1e-06
logit_scale = 20.0
log2_e = 1.4426950408889634
ln_2 = 0.6931471805599453


f32 = jnp.float32
bf16 = jnp.bfloat16
VMEM = pl.BlockSpec(memory_space=pltpu.VMEM)
SMEM = pl.BlockSpec(memory_space=pltpu.SMEM)
ANY = pl.BlockSpec(memory_space=pl.ANY)
MIB = 1 << 20
zero_rows = 8
bags_at_once = 8


def widen_kernel(pieces, groups, table_ref, ids_ref, lengths_ref, wide_ref, *refs):
    raw, ids, lengths, table_sems, sems = refs[-5:]
    rows = table_ref.shape[0]
    piece = rows // pieces
    block = min(256, piece)
    copies = [
        pltpu.make_async_copy(
            table_ref.at[pl.ds(k * piece, piece)], raw.at[pl.ds(k * piece, piece)], table_sems.at[k]
        )
        for k in range(pieces)
    ]
    bags = [
        pltpu.make_async_copy(ids_ref, ids, sems.at[0]),
        pltpu.make_async_copy(lengths_ref, lengths, sems.at[1]),
    ]
    for copy in copies[:1] + bags + copies[1:]:
        copy.start()
    wide_ref[pl.ds(rows, zero_rows), :] = jnp.zeros((zero_rows, wide_ref.shape[1]), f32)
    for copy in bags:
        copy.wait()
    if groups:
        places_ref, inverse_ref = refs[:2]
        T, C, run = groups
        positions = ids.shape[0]
        local = ids[...] - lax.axis_index("tab") * rows
        valid = lax.broadcasted_iota(jnp.int32, ids.shape, 0) < lengths[...]
        places = jnp.where((local >= 0) & (local < rows) & valid, local, rows)
        inverse = 1.0 / lengths[...].astype(f32)
        for t in range(T):
            for c in range(C):
                at = (t * C + c) * run
                to = pl.ds(c * positions * T + t, positions, stride=T)
                places_ref[to, :] = places[:, at : at + run]
                inverse_ref[pl.ds(c * T + t, 1), :] = inverse[:, at : at + run]
    for k in range(pieces):
        copies[k].wait()

        @pl.loop(0, piece // block)
        def _(i):
            at = pl.ds(pl.multiple_of(k * piece + i * block, block), block)
            wide_ref[at, :] = raw[at, :].astype(f32)


def widen(table, ids, lengths, T, C):
    rows, width = table.shape
    positions, items = ids.shape
    pieces = 8
    run = items // (T * C)
    groups = (T, C, run) if run % 128 == 0 else None
    extra = ()
    if groups:
        extra = (
            jax.ShapeDtypeStruct((C * positions * T, run), jnp.int32),
            jax.ShapeDtypeStruct((C * T, run), f32),
        )
    hbm = pl.BlockSpec(memory_space=pltpu.HBM)
    wide, *rest = pl.pallas_call(
        functools.partial(widen_kernel, pieces, groups),
        out_shape=(pltpu.VMEM((rows + zero_rows, width), f32),) + extra,
        in_specs=[hbm, hbm, hbm],
        out_specs=(VMEM,) * (1 + len(extra)),
        scratch_shapes=[
            pltpu.VMEM((rows, width), bf16),
            pltpu.VMEM(ids.shape, jnp.int32),
            pltpu.VMEM(lengths.shape, jnp.int32),
            pltpu.SemaphoreType.DMA((pieces,)),
            pltpu.SemaphoreType.DMA((2,)),
        ],
        compiler_params=pltpu.CompilerParams(vmem_limit_bytes=30 * MIB),
        cost_estimate=pl.CostEstimate(flops=10**6, bytes_accessed=rows * width * 2, transcendentals=0),
        name="widen",
    )(table, ids, lengths)
    if groups:
        return wide, rest[0].reshape(-1), rest[1].reshape(-1)
    local = ids - lax.axis_index("tab") * rows
    valid = lax.broadcasted_iota(jnp.int32, ids.shape, 0) < lengths
    places = jnp.where((local >= 0) & (local < rows) & valid, local, rows)
    places = places.reshape(positions, T, C, run).transpose(2, 0, 1, 3).reshape(-1)
    inverse = (1.0 / lengths.astype(f32)).reshape(T, C, run).transpose(1, 0, 2).reshape(-1)
    return wide, places, inverse


def pool_kernel(positions, ahead, inverse_ref, wide_ref, places_ref, after_ref, out_ref, places, inverse, sems):
    count = out_ref.shape[0]
    chunk = lax.rem(lax.axis_index("cand") + ahead, lax.axis_size("cand"))
    start = pl.multiple_of(chunk * (count * positions), count * positions)
    copies = [
        pltpu.make_async_copy(places_ref.at[pl.ds(start, count * positions)], places, sems.at[0]),
        pltpu.make_async_copy(inverse_ref, inverse, sems.at[1]),
    ]
    for copy in copies:
        copy.start()
    for copy in copies:
        copy.wait()

    @pl.loop(0, count // bags_at_once)
    def _(b):
        for u in range(bags_at_once):
            i = b * bags_at_once + u
            rows = [
                wide_ref[pl.ds(places.at[pl.ds(p * count, count)][i], 1), :] for p in range(positions)
            ]
            while len(rows) > 1:
                rows = [sum(rows[k : k + 2][1:], rows[k]) for k in range(0, len(rows), 2)]
            out_ref[pl.ds(i, 1), :] = rows[0] * inverse[chunk * count + i]


def pool(ahead, inverse, wide, places, after, count, positions):
    width = wide.shape[1]
    return pl.pallas_call(
        functools.partial(pool_kernel, positions, ahead),
        out_shape=jax.ShapeDtypeStruct((count, width), f32),
        in_specs=[ANY, VMEM, ANY, ANY],
        out_specs=VMEM,
        scratch_shapes=[
            pltpu.SMEM((count * positions,), jnp.int32),
            pltpu.SMEM(inverse.shape, f32),
            pltpu.SemaphoreType.DMA((2,)),
        ],
        compiler_params=pltpu.CompilerParams(vmem_limit_bytes=20 * MIB),
        cost_estimate=pl.CostEstimate(flops=10**7, bytes_accessed=count * width * 4, transcendentals=0),
        name="pool%d" % ahead,
    )(inverse, wide, places, after)


def project_kernel(order, *refs):
    count = len(order)
    parts, weight_ref, send_ref, keep_ref = refs[:count], refs[count], refs[-2], refs[-1]
    half = send_ref.shape[0]
    width = parts[0].shape[1]
    c, d = lax.axis_index("cand"), lax.axis_index("dp")
    C, D = lax.axis_size("cand"), lax.axis_size("dp")
    own_half = lax.rem(d, 2)
    for which, out_ref in ((1 - own_half, send_ref), (own_half, keep_ref)):
        at = pl.ds(pl.multiple_of(which * half, half), half)
        total = None
        for k in range(count):
            value = parts[k][at, :]
            source = lax.rem(c + C - order[k], C) * D + d
            weight = weight_ref[pl.ds(pl.multiple_of(source * width, width), width), :]
            for _ in range(3):
                short = value.astype(bf16)
                term = jnp.dot(short, weight, preferred_element_type=f32)
                total = term if total is None else total + term
                value = value - short.astype(f32)
        out_ref[...] = total


def project(order, parts, weight):
    rows = parts[0].shape[0]
    shape = jax.ShapeDtypeStruct((rows // 2, weight.shape[1]), f32)
    return pl.pallas_call(
        functools.partial(project_kernel, order),
        out_shape=(shape, shape),
        in_specs=[VMEM] * (len(parts) + 1),
        out_specs=(VMEM, VMEM),
        compiler_params=pltpu.CompilerParams(vmem_limit_bytes=8 * MIB),
        cost_estimate=pl.CostEstimate(flops=10**8, bytes_accessed=2 * MIB, transcendentals=0),
        name="project",
    )(*parts, weight)


def tower_kernel(block, features_ref, w1_ref, w2_ref, after_ref, high_ref, low_ref):
    for start in range(0, features_ref.shape[0], block):
        at = pl.ds(start, block)
        hidden = jnp.dot(features_ref[at, :], w1_ref[...], preferred_element_type=f32)
        hidden = 0.5 * hidden * (1.0 + lax.erf(hidden * (0.5**0.5)))
        emb = jnp.dot(hidden.astype(bf16), w2_ref[...], preferred_element_type=f32)
        emb = emb * lax.rsqrt(jnp.mean(emb * emb, axis=1, keepdims=True) + epsilon)
        high = emb.astype(bf16)
        high_ref[at, :] = high
        low_ref[at, :] = (emb - high.astype(f32)).astype(bf16)


def tower(part, parts, features, w1, w2, after):
    users = features.shape[0] // parts
    embed = w2.shape[1]
    whole = lambda i: (0, 0)
    shape = jax.ShapeDtypeStruct((users, embed), bf16)
    return pl.pallas_call(
        functools.partial(tower_kernel, min(256, users)),
        grid=(1,),
        out_shape=(shape, shape),
        in_specs=[
            pl.BlockSpec((users, features.shape[1]), lambda i: (part, 0)),
            VMEM,
            VMEM,
            ANY,
        ],
        out_specs=(pl.BlockSpec((users, embed), whole), pl.BlockSpec((users, embed), whole)),
        compiler_params=pltpu.CompilerParams(vmem_limit_bytes=16 * MIB),
        cost_estimate=pl.CostEstimate(
            flops=2 * users * (w1.size + w2.size), bytes_accessed=2 * MIB, transcendentals=users * w1.shape[1]
        ),
        name="tower%d" % part,
    )(features, w1, w2, after)


def split(x, size):
    if size & (size - 1) == 0:
        return x >> (size.bit_length() - 1), x & (size - 1)
    return lax.div(x, jnp.full_like(x, size)), lax.rem(x, jnp.full_like(x, size))


def scores_kernel(count, block, own, positive_ref, mine_ref, other_ref, *refs):
    item_ref, out_ref = refs[-2:]
    t, c, d = (lax.axis_index(axis) for axis in ("tab", "cand", "dp"))
    C, D = lax.axis_size("cand"), lax.axis_size("dp")
    half = mine_ref.shape[0]
    first = lax.rem(d, 2) * half
    items = jnp.concatenate([mine_ref[...], other_ref[...]], axis=0)
    items = items * (logit_scale / items.shape[1] * log2_e)
    item_high = items.astype(bf16)
    item_low = (items - item_high.astype(f32)).astype(bf16)
    users = refs[0].shape[0]

    def dot(a, b):
        return lax.dot_general(a, b, (((1,), (1,)), ((), ())), preferred_element_type=f32)

    for k in range(count):
        high_ref, low_ref = refs[2 * k], refs[2 * k + 1]
        for start in range(0, users, block):
            at = pl.ds(start, block)
            high = high_ref[at, :]
            scores = dot(item_high, high) + (dot(item_low, high) + dot(item_high, low_ref[at, :]))
            to = pl.ds(k * users + start, block)
            rest, within = split(positive_ref[:, to], own)
            rest, owner_d = split(rest, D)
            owner_t, owner_c = split(rest, C)
            place = (owner_t * D + owner_d) * own + within - first
            place = jnp.where(place < 0, place + 2 * half, place)
            place = jnp.where(owner_c == c, place, -1)
            here = lax.broadcasted_iota(jnp.int32, scores.shape, 0) == place
            out_ref[pl.ds(0, 1), to] = jnp.sum(jnp.exp2(scores), axis=0, keepdims=True)
            out_ref[pl.ds(1, 1), to] = jnp.sum(
                jnp.where(here, scores, 0.0), axis=0, keepdims=True
            )
    row = (t * D + d) * own - first
    inside = (row >= 0) & (row < half)

    step = 8 if own % 8 == 0 else 1

    def copy_rows(from_ref, start):
        for k in range(0, own, step):
            at = pl.ds(pl.multiple_of(start + k, step), step)
            item_ref[pl.ds(k, step), :] = from_ref[at, :]

    @pl.when(inside)
    def _():
        copy_rows(mine_ref, row)

    @pl.when(jnp.logical_not(inside))
    def _():
        copy_rows(other_ref, lax.rem(row + 2 * half, half))


def score(positives, mine, other, embs, own):
    count = len(embs)
    users = embs[0][0].shape[0]
    flat = [x for pair in embs for x in pair]
    total = users * count
    return pl.pallas_call(
        functools.partial(scores_kernel, count, min(512, users), own),
        out_shape=(
            jax.ShapeDtypeStruct((own, mine.shape[1]), f32),
            jax.ShapeDtypeStruct((2, total), f32),
        ),
        in_specs=[VMEM] * (3 + len(flat)),
        out_specs=(VMEM, VMEM),
        compiler_params=pltpu.CompilerParams(vmem_limit_bytes=16 * MIB),
        cost_estimate=pl.CostEstimate(
            flops=6 * total * mine.shape[1] * 2 * mine.shape[0], bytes_accessed=2 * MIB, transcendentals=0
        ),
        name="score",
    )(positives, mine, other, *flat)


def swap(x, axis, bit):
    return lax.ppermute(x, axis, [(i, i ^ bit) for i in range(lax.axis_size(axis))])


def shift(x, axis, by):
    size = lax.axis_size(axis)
    return lax.ppermute(x, axis, [(i, (i + by) % size) for i in range(size)])


def bits_of(axis):
    return [(axis, 1 << k) for k in range(lax.axis_size(axis).bit_length() - 1)]


def body(
    tables, bag_ids, bag_lengths, item_weight, user_features, user_w1, user_w2, positive_items
):
    table = tables[0]
    ids = bag_ids[0].T
    T, C, D = lax.axis_size("tab"), lax.axis_size("cand"), lax.axis_size("dp")
    positions, items = ids.shape
    own = items // (T * C * D)
    count = items // C
    half = count // 2

    wide, places, inverse = widen(table, ids, bag_lengths, T, C)
    order = sorted(range(1, C), key=lambda j: -min(j, C - j)) + [0]
    after = places
    received = []
    for j in order:
        part = pool(j, inverse, wide, places, after, count, positions)
        after = part
        received.append(shift(part, "cand", j) if j else part)

    tower_parts = 4
    embs = [tower(k, tower_parts, user_features, user_w1, user_w2, after) for k in range(tower_parts // 2)]
    send, keep = project(order, received, item_weight)
    embs += [
        tower(k, tower_parts, user_features, user_w1, user_w2, keep)
        for k in range(tower_parts // 2, tower_parts)
    ]
    total = keep + swap(send, "dp", 1)
    others = [step for step in bits_of("dp") if step[1] > 1] + bits_of("tab")
    quarter = half // 2
    pieces = [total[:quarter], total[quarter:]]
    turned = others[len(others) // 2 :] + others[: len(others) // 2]
    for step_a, step_b in zip(others, turned):
        moved = [swap(pieces[0], *step_a), swap(pieces[1], *step_b)]
        pieces = [a + b for a, b in zip(pieces, moved)]
    total = jnp.concatenate(pieces, axis=0)
    mine = total * lax.rsqrt(jnp.mean(total * total, axis=1, keepdims=True) + epsilon)
    other = swap(mine, "dp", 1)

    item_emb, partial = score(positive_items[None], mine, other, embs, own)
    summed = partial
    for j in range(1, C):
        summed = summed + shift(partial, "cand", j)
    user_loss = (jnp.log2(summed[0]) - summed[1]) * ln_2
    return (item_emb, user_loss)


def solution(mesh):
    placed = (
        P(("cand", "dp"), "tab", None),
        P(("cand", "dp"), None, None),
        P(("cand", "dp"), None),
        P(),
        P(("tab", "dp"), None),
        P(),
        P(),
        P(("tab", "dp")),
    )
    return jax.shard_map(
        body,
        mesh=mesh,
        in_specs=placed,
        out_specs=(P(("tab", "cand", "dp"), None), P(("tab", "dp"))),
        check_vma=False,
    )
```

```python
import functools

import jax
import jax.numpy as jnp
from jax import lax
from jax.experimental import pallas as pl
from jax.experimental.pallas import tpu as pltpu
from jax.sharding import PartitionSpec as P


epsilon = 1e-06
logit_scale = 20.0
log2_e = 1.4426950408889634
ln_2 = 0.6931471805599453


f32 = jnp.float32
bf16 = jnp.bfloat16
VMEM = pl.BlockSpec(memory_space=pltpu.VMEM)
SMEM = pl.BlockSpec(memory_space=pltpu.SMEM)
ANY = pl.BlockSpec(memory_space=pl.ANY)
MIB = 1 << 20
zero_rows = 8
bags_at_once = 8
tower_parts = 4


def widen_kernel(pieces, table_ref, wide_ref, raw, sems):
    rows = table_ref.shape[0]
    piece = rows // pieces
    block = min(256, piece)
    copies = [
        pltpu.make_async_copy(
            table_ref.at[pl.ds(k * piece, piece)], raw.at[pl.ds(k * piece, piece)], sems.at[k]
        )
        for k in range(pieces)
    ]
    for copy in copies:
        copy.start()
    wide_ref[pl.ds(rows, zero_rows), :] = jnp.zeros((zero_rows, wide_ref.shape[1]), f32)
    for k in range(pieces):
        copies[k].wait()

        @pl.loop(0, piece // block)
        def _(i):
            at = pl.ds(pl.multiple_of(k * piece + i * block, block), block)
            wide_ref[at, :] = raw[at, :].astype(f32)


def widen(table):
    rows, width = table.shape
    pieces = 16
    return pl.pallas_call(
        functools.partial(widen_kernel, pieces),
        out_shape=pltpu.VMEM((rows + zero_rows, width), f32),
        in_specs=[pl.BlockSpec(memory_space=pltpu.HBM)],
        out_specs=VMEM,
        scratch_shapes=[pltpu.VMEM((rows, width), bf16), pltpu.SemaphoreType.DMA((pieces,))],
        compiler_params=pltpu.CompilerParams(vmem_limit_bytes=30 * MIB),
        cost_estimate=pl.CostEstimate(flops=10**6, bytes_accessed=rows * width * 2, transcendentals=0),
        name="widen",
    )(table)


def place_kernel(T, C, rows, ids_ref, lengths_ref, after_ref, places_ref, inverse_ref):
    positions, items = ids_ref.shape
    run = items // (T * C)
    local = ids_ref[...] - lax.axis_index("tab") * rows
    valid = lax.broadcasted_iota(jnp.int32, local.shape, 0) < lengths_ref[...]
    places = jnp.where((local >= 0) & (local < rows) & valid, local, rows)
    inverse = 1.0 / lengths_ref[...].astype(f32)
    for t in range(T):
        for c in range(C):
            at = (t * C + c) * run
            to = pl.ds(c * positions * T + t, positions, stride=T)
            places_ref[to, :] = places[:, at : at + run]
            inverse_ref[pl.ds(c * T + t, 1), :] = inverse[:, at : at + run]


def place(ids, lengths, wide, T, C):
    positions, items = ids.shape
    rows = wide.shape[0] - zero_rows
    run = items // (T * C)
    if run % 128 == 0:
        places, inverse = pl.pallas_call(
            functools.partial(place_kernel, T, C, rows),
            out_shape=(
                jax.ShapeDtypeStruct((C * positions * T, run), jnp.int32),
                jax.ShapeDtypeStruct((C * T, run), f32),
            ),
            in_specs=[VMEM, VMEM, ANY],
            out_specs=(VMEM, VMEM),
            compiler_params=pltpu.CompilerParams(vmem_limit_bytes=4 * MIB),
            name="place",
        )(ids, lengths, wide)
        return places.reshape(-1), inverse.reshape(-1)
    local = ids - lax.axis_index("tab") * rows
    valid = lax.broadcasted_iota(jnp.int32, ids.shape, 0) < lengths
    places = jnp.where((local >= 0) & (local < rows) & valid, local, rows)
    places = places.reshape(positions, T, C, run).transpose(2, 0, 1, 3).reshape(-1)
    inverse = (1.0 / lengths.astype(f32)).reshape(T, C, run).transpose(1, 0, 2).reshape(-1)
    return places, inverse


def pool_kernel(positions, aheads, inverse_ref, wide_ref, places_ref, after_ref, *refs):
    count = refs[0].shape[0]
    out_refs = refs[: len(aheads)]
    places, inverse, sems = refs[len(aheads) :]
    size = count * positions
    chunks = [lax.rem(lax.axis_index("cand") + j, lax.axis_size("cand")) for j in aheads]
    copies = [pltpu.make_async_copy(inverse_ref, inverse, sems.at[0])]
    for k, chunk in enumerate(chunks):
        start = pl.multiple_of(chunk * size, size)
        copies.append(
            pltpu.make_async_copy(
                places_ref.at[pl.ds(start, size)], places.at[pl.ds(k * size, size)], sems.at[k + 1]
            )
        )
    for copy in copies:
        copy.start()
    copies[0].wait()
    for k, chunk in enumerate(chunks):
        copies[k + 1].wait()
        out_ref = out_refs[k]

        @pl.loop(0, count // bags_at_once)
        def _(b):
            for u in range(bags_at_once):
                i = b * bags_at_once + u
                rows = [
                    wide_ref[pl.ds(places.at[pl.ds(k * size + p * count, count)][i], 1), :]
                    for p in range(positions)
                ]
                while len(rows) > 1:
                    rows = [sum(rows[n : n + 2][1:], rows[n]) for n in range(0, len(rows), 2)]
                out_ref[pl.ds(i, 1), :] = rows[0] * inverse[chunk * count + i]


def pool(aheads, inverse, wide, places, after, count, positions):
    width = wide.shape[1]
    return pl.pallas_call(
        functools.partial(pool_kernel, positions, aheads),
        out_shape=(jax.ShapeDtypeStruct((count, width), f32),) * len(aheads),
        in_specs=[ANY, VMEM, ANY, ANY],
        out_specs=(VMEM,) * len(aheads),
        scratch_shapes=[
            pltpu.SMEM((len(aheads) * count * positions,), jnp.int32),
            pltpu.SMEM(inverse.shape, f32),
            pltpu.SemaphoreType.DMA((len(aheads) + 1,)),
        ],
        compiler_params=pltpu.CompilerParams(vmem_limit_bytes=20 * MIB),
        cost_estimate=pl.CostEstimate(
            flops=10**7 * len(aheads), bytes_accessed=count * width * 4, transcendentals=0
        ),
        name="pool",
    )(inverse, wide, places, after)


def project_kernel(order, *refs):
    count = len(order)
    parts, weight_ref, send_ref, keep_ref = refs[:count], refs[count], refs[-2], refs[-1]
    half = send_ref.shape[0]
    width = parts[0].shape[1]
    c, d = lax.axis_index("cand"), lax.axis_index("dp")
    C, D = lax.axis_size("cand"), lax.axis_size("dp")
    own_half = lax.rem(d, 2)
    for which, out_ref in ((1 - own_half, send_ref), (own_half, keep_ref)):
        at = pl.ds(pl.multiple_of(which * half, half), half)
        total = None
        for k in range(count):
            value = parts[k][at, :]
            source = lax.rem(c + C - order[k], C) * D + d
            weight = weight_ref[pl.ds(pl.multiple_of(source * width, width), width), :]
            for _ in range(3):
                short = value.astype(bf16)
                term = jnp.dot(short, weight, preferred_element_type=f32)
                total = term if total is None else total + term
                value = value - short.astype(f32)
        out_ref[...] = total


def project(order, parts, weight):
    rows = parts[0].shape[0]
    shape = jax.ShapeDtypeStruct((rows // 2, weight.shape[1]), f32)
    return pl.pallas_call(
        functools.partial(project_kernel, order),
        out_shape=(shape, shape),
        in_specs=[VMEM] * (len(parts) + 1),
        out_specs=(VMEM, VMEM),
        compiler_params=pltpu.CompilerParams(vmem_limit_bytes=8 * MIB),
        cost_estimate=pl.CostEstimate(flops=10**8, bytes_accessed=2 * MIB, transcendentals=0),
        name="project",
    )(*parts, weight)


def tower_kernel(block, features_ref, w1_ref, w2_ref, after_ref, high_ref, low_ref):
    for start in range(0, features_ref.shape[0], block):
        at = pl.ds(start, block)
        hidden = jnp.dot(features_ref[at, :], w1_ref[...], preferred_element_type=f32)
        hidden = 0.5 * hidden * (1.0 + lax.erf(hidden * (0.5**0.5)))
        emb = jnp.dot(hidden.astype(bf16), w2_ref[...], preferred_element_type=f32)
        emb = emb * lax.rsqrt(jnp.mean(emb * emb, axis=1, keepdims=True) + epsilon)
        high = emb.astype(bf16)
        high_ref[at, :] = high
        low_ref[at, :] = (emb - high.astype(f32)).astype(bf16)


def tower(part, parts, features, w1, w2, after):
    users = features.shape[0] // parts
    embed = w2.shape[1]
    whole = lambda i: (0, 0)
    shape = jax.ShapeDtypeStruct((users, embed), bf16)
    return pl.pallas_call(
        functools.partial(tower_kernel, min(256, users)),
        grid=(1,),
        out_shape=(shape, shape),
        in_specs=[
            pl.BlockSpec((users, features.shape[1]), lambda i: (part, 0)),
            VMEM,
            VMEM,
            ANY,
        ],
        out_specs=(pl.BlockSpec((users, embed), whole), pl.BlockSpec((users, embed), whole)),
        compiler_params=pltpu.CompilerParams(vmem_limit_bytes=16 * MIB),
        cost_estimate=pl.CostEstimate(
            flops=2 * users * (w1.size + w2.size), bytes_accessed=2 * MIB, transcendentals=users * w1.shape[1]
        ),
    )(features, w1, w2, after)


def split(x, size):
    if size & (size - 1) == 0:
        return x >> (size.bit_length() - 1), x & (size - 1)
    return lax.div(x, jnp.full_like(x, size)), lax.rem(x, jnp.full_like(x, size))


def scores_kernel(count, block, own, positive_ref, mine_ref, other_ref, *refs):
    item_ref, out_ref = refs[-2:]
    t, c, d = (lax.axis_index(axis) for axis in ("tab", "cand", "dp"))
    C, D = lax.axis_size("cand"), lax.axis_size("dp")
    half = mine_ref.shape[0]
    first = lax.rem(d, 2) * half
    items = jnp.concatenate([mine_ref[...], other_ref[...]], axis=0)
    items = items * (logit_scale / items.shape[1] * log2_e)
    item_high = items.astype(bf16)
    item_low = (items - item_high.astype(f32)).astype(bf16)
    users = refs[0].shape[0]

    def dot(a, b):
        return lax.dot_general(a, b, (((1,), (1,)), ((), ())), preferred_element_type=f32)

    for k in range(count):
        high_ref, low_ref = refs[2 * k], refs[2 * k + 1]
        for start in range(0, users, block):
            at = pl.ds(start, block)
            high = high_ref[at, :]
            scores = dot(item_high, high) + (dot(item_low, high) + dot(item_high, low_ref[at, :]))
            to = pl.ds(k * users + start, block)
            rest, within = split(positive_ref[:, to], own)
            rest, owner_d = split(rest, D)
            owner_t, owner_c = split(rest, C)
            place = (owner_t * D + owner_d) * own + within - first
            place = jnp.where(place < 0, place + 2 * half, place)
            place = jnp.where(owner_c == c, place, -1)
            here = lax.broadcasted_iota(jnp.int32, scores.shape, 0) == place
            out_ref[pl.ds(0, 1), to] = jnp.sum(jnp.exp2(scores), axis=0, keepdims=True)
            out_ref[pl.ds(1, 1), to] = jnp.sum(
                jnp.where(here, scores, 0.0), axis=0, keepdims=True
            )
    row = (t * D + d) * own - first
    inside = (row >= 0) & (row < half)

    step = 8 if own % 8 == 0 else 1

    def copy_rows(from_ref, start):
        for k in range(0, own, step):
            at = pl.ds(pl.multiple_of(start + k, step), step)
            item_ref[pl.ds(k, step), :] = from_ref[at, :]

    @pl.when(inside)
    def _():
        copy_rows(mine_ref, row)

    @pl.when(jnp.logical_not(inside))
    def _():
        copy_rows(other_ref, lax.rem(row + 2 * half, half))


def score(positives, mine, other, embs, own):
    count = len(embs)
    users = embs[0][0].shape[0]
    flat = [x for pair in embs for x in pair]
    total = users * count
    return pl.pallas_call(
        functools.partial(scores_kernel, count, min(512, users), own),
        out_shape=(
            jax.ShapeDtypeStruct((own, mine.shape[1]), f32),
            jax.ShapeDtypeStruct((2, total), f32),
        ),
        in_specs=[VMEM] * (3 + len(flat)),
        out_specs=(VMEM, VMEM),
        compiler_params=pltpu.CompilerParams(vmem_limit_bytes=16 * MIB),
        cost_estimate=pl.CostEstimate(
            flops=6 * total * mine.shape[1] * 2 * mine.shape[0], bytes_accessed=2 * MIB, transcendentals=0
        ),
        name="score",
    )(positives, mine, other, *flat)


def swap(x, axis, bit):
    return lax.ppermute(x, axis, [(i, i ^ bit) for i in range(lax.axis_size(axis))])


def swap_both(x, bit_dp, bit_tab):
    T, D = lax.axis_size("tab"), lax.axis_size("dp")
    pairs = [(t * D + d, (t ^ bit_tab) * D + (d ^ bit_dp)) for t in range(T) for d in range(D)]
    return lax.ppermute(x, ("tab", "dp"), pairs)


def shift(x, axis, by):
    size = lax.axis_size(axis)
    return lax.ppermute(x, axis, [(i, (i + by) % size) for i in range(size)])


def bits_of(axis):
    return [(axis, 1 << k) for k in range(lax.axis_size(axis).bit_length() - 1)]


def body(
    tables, bag_ids, bag_lengths, item_weight, user_features, user_w1, user_w2, positive_items
):
    table = tables[0]
    ids = bag_ids[0].T
    T, C, D = lax.axis_size("tab"), lax.axis_size("cand"), lax.axis_size("dp")
    positions, items = ids.shape
    own = items // (T * C * D)
    count = items // C

    wide = widen(table)
    places, inverse = place(ids, bag_lengths, wide, T, C)
    groups = pool_groups(C)
    order = sum(groups, ())
    after = places
    received = []
    for group in groups:
        parts = pool(group, inverse, wide, places, after, count, positions)
        after = parts[-1]
        for j, part in zip(group, parts):
            if j:
                part = shift(part, "cand", j)
            received.append(part)

    send, keep = project(order, received, item_weight)
    total = keep + swap(send, "dp", 1)
    embs = []
    for k in range(tower_parts):
        embs.append(tower(k, tower_parts, user_features, user_w1, user_w2, keep))
    steps = [step for step in bits_of("dp") if step[1] > 1] + bits_of("tab")
    if len(steps) == 2:
        moved = []
        for picked in ((1, 1), (1, 0), (0, 1)):
            moved.append(swap_both(total, picked[0] * steps[0][1], picked[1] * steps[1][1]))
        total = (total + moved[1]) + (moved[2] + moved[0])
    else:
        for step in steps:
            total = total + swap(total, *step)
    mine = total * lax.rsqrt(jnp.mean(total * total, axis=1, keepdims=True) + epsilon)
    other = swap(mine, "dp", 1)
    item_emb, partial = score(positive_items[None], mine, other, embs, own)
    summed = partial
    for j in range(1, C):
        summed = summed + swap(partial, "cand", j)
    user_loss = (jnp.log2(summed[0]) - summed[1]) * ln_2
    return (item_emb, user_loss)


def pool_groups(C):
    order = sorted(range(1, C), key=lambda j: -min(j, C - j))
    return tuple(group for group in ((order[0],), tuple(order[1:]), (0,)) if group)


def solution(mesh):
    placed = (
        P(("cand", "dp"), "tab", None),
        P(("cand", "dp"), None, None),
        P(("cand", "dp"), None),
        P(),
        P(("tab", "dp"), None),
        P(),
        P(),
        P(("tab", "dp")),
    )
    return jax.shard_map(
        body,
        mesh=mesh,
        in_specs=placed,
        out_specs=(P(("tab", "cand", "dp"), None), P(("tab", "dp"))),
        check_vma=False,
    )
```

```python
import functools

import jax
import jax.numpy as jnp
from jax import lax
from jax.experimental import pallas as pl
from jax.experimental.pallas import tpu as pltpu
from jax.sharding import PartitionSpec as P


epsilon = 1e-06
logit_scale = 20.0
log2_e = 1.4426950408889634
ln_2 = 0.6931471805599453


f32 = jnp.float32
bf16 = jnp.bfloat16
VMEM = pl.BlockSpec(memory_space=pltpu.VMEM)
SMEM = pl.BlockSpec(memory_space=pltpu.SMEM)
ANY = pl.BlockSpec(memory_space=pl.ANY)
MIB = 1 << 20
zero_rows = 8
bags_at_once = 16
tower_parts = 4


def widen_kernel(pieces, table_ref, wide_ref, raw, sems):
    rows = table_ref.shape[0]
    piece = rows // pieces
    block = min(1024, piece)
    copies = [
        pltpu.make_async_copy(
            table_ref.at[pl.ds(k * piece, piece)], raw.at[pl.ds(k * piece, piece)], sems.at[k]
        )
        for k in range(pieces)
    ]
    for copy in copies:
        copy.start()
    wide_ref[pl.ds(rows, zero_rows), :] = jnp.zeros((zero_rows, wide_ref.shape[1]), f32)
    for k in range(pieces):
        copies[k].wait()

        @pl.loop(0, piece // block)
        def _(i):
            at = pl.ds(pl.multiple_of(k * piece + i * block, block), block)
            wide_ref[at, :] = raw[at, :].astype(f32)


def widen(table):
    rows, width = table.shape
    pieces = 16
    return pl.pallas_call(
        functools.partial(widen_kernel, pieces),
        out_shape=pltpu.VMEM((rows + zero_rows, width), f32),
        in_specs=[pl.BlockSpec(memory_space=pltpu.HBM)],
        out_specs=VMEM,
        scratch_shapes=[pltpu.VMEM((rows, width), bf16), pltpu.SemaphoreType.DMA((pieces,))],
        compiler_params=pltpu.CompilerParams(vmem_limit_bytes=30 * MIB),
        cost_estimate=pl.CostEstimate(flops=10**6, bytes_accessed=rows * width * 2, transcendentals=0),
        name="widen",
    )(table)


def place_kernel(T, C, rows, ids_ref, lengths_ref, after_ref, places_ref, inverse_ref):
    positions, items = ids_ref.shape
    run = items // (T * C)
    local = ids_ref[...] - lax.axis_index("tab") * rows
    valid = lax.broadcasted_iota(jnp.int32, local.shape, 0) < lengths_ref[...]
    places = jnp.where((local >= 0) & (local < rows) & valid, local, rows)
    inverse = 1.0 / lengths_ref[...].astype(f32)
    for t in range(T):
        for c in range(C):
            at = (t * C + c) * run
            to = pl.ds((c * T + t) * positions, positions)
            places_ref[to, :] = places[:, at : at + run]
            inverse_ref[pl.ds(c * T + t, 1), :] = inverse[:, at : at + run]


def place(ids, lengths, wide, T, C):
    positions, items = ids.shape
    rows = wide.shape[0] - zero_rows
    run = items // (T * C)
    if run % 128 == 0:
        places, inverse = pl.pallas_call(
            functools.partial(place_kernel, T, C, rows),
            out_shape=(
                jax.ShapeDtypeStruct((C * positions * T, run), jnp.int32),
                jax.ShapeDtypeStruct((C * T, run), f32),
            ),
            in_specs=[VMEM, VMEM, ANY],
            out_specs=(VMEM, VMEM),
            compiler_params=pltpu.CompilerParams(vmem_limit_bytes=4 * MIB),
            name="place",
        )(ids, lengths, wide)
        return places.reshape(-1), inverse.reshape(-1)
    local = ids - lax.axis_index("tab") * rows
    valid = lax.broadcasted_iota(jnp.int32, ids.shape, 0) < lengths
    places = jnp.where((local >= 0) & (local < rows) & valid, local, rows)
    places = places.reshape(positions, T, C, run).transpose(2, 1, 0, 3).reshape(-1)
    inverse = (1.0 / lengths.astype(f32)).reshape(T, C, run).transpose(1, 0, 2).reshape(-1)
    return places, inverse


def pool_kernel(positions, run, ahead, inverse_ref, wide_ref, places_ref, after_ref, out_ref, *refs):
    places, inverse, sems = refs
    count = out_ref.shape[0]
    size = count * positions
    pieces = sems.shape[0] - 1
    chunk = lax.rem(lax.axis_index("cand") + ahead, lax.axis_size("cand"))
    copies = [pltpu.make_async_copy(inverse_ref, inverse, sems.at[pieces])]
    for k in range(pieces):
        piece = size // pieces
        start = pl.multiple_of(chunk * size + k * piece, piece)
        copies.append(
            pltpu.make_async_copy(
                places_ref.at[pl.ds(start, piece)], places.at[pl.ds(k * piece, piece)], sems.at[k]
            )
        )
    for copy in copies:
        copy.start()
    copies[0].wait()
    at_once = min(bags_at_once, run)
    for t in range(count // run):
        if t < pieces:
            copies[t + 1].wait()
        index_refs = [places.at[pl.ds((t * positions + p) * run, run)] for p in range(positions)]

        @pl.loop(0, run // at_once)
        def _(b):
            for u in range(at_once):
                i = b * at_once + u
                rows = [wide_ref[pl.ds(ref[i], 1), :] for ref in index_refs]
                while len(rows) > 1:
                    rows = [sum(rows[n : n + 2][1:], rows[n]) for n in range(0, len(rows), 2)]
                scale = inverse[chunk * count + t * run + i]
                out_ref[pl.ds(t * run + i, 1), :] = rows[0] * scale


def pool(ahead, inverse, wide, places, after, count, positions, run):
    width = wide.shape[1]
    pieces = count // run if positions * run % 1024 == 0 else 1
    return pl.pallas_call(
        functools.partial(pool_kernel, positions, run, ahead),
        out_shape=jax.ShapeDtypeStruct((count, width), f32),
        in_specs=[ANY, VMEM, ANY, ANY],
        out_specs=VMEM,
        scratch_shapes=[
            pltpu.SMEM((count * positions,), jnp.int32),
            pltpu.SMEM(inverse.shape, f32),
            pltpu.SemaphoreType.DMA((pieces + 1,)),
        ],
        compiler_params=pltpu.CompilerParams(vmem_limit_bytes=20 * MIB),
        cost_estimate=pl.CostEstimate(
            flops=10**7, bytes_accessed=count * width * 4, transcendentals=0
        ),
        name="pool",
    )(inverse, wide, places, after)


def project_kernel(order, other, *refs):
    count = len(order)
    parts, weight_ref, out_ref = refs[:count], refs[count], refs[-1]
    half = out_ref.shape[0]
    width = parts[0].shape[1]
    c, d = lax.axis_index("cand"), lax.axis_index("dp")
    C, D = lax.axis_size("cand"), lax.axis_size("dp")
    which = lax.rem(d + other, 2)
    at = pl.ds(pl.multiple_of(which * half, half), half)
    total = None
    for k in range(count):
        value = parts[k][at, :]
        source = lax.rem(c + C - order[k], C) * D + d
        weight = weight_ref[pl.ds(pl.multiple_of(source * width, width), width), :]
        for _ in range(3):
            short = value.astype(bf16)
            term = jnp.dot(short, weight, preferred_element_type=f32)
            total = term if total is None else total + term
            value = value - short.astype(f32)
    out_ref[...] = total


def project(order, other, parts, weight, after):
    rows = parts[0].shape[0]
    return pl.pallas_call(
        functools.partial(project_kernel, order, other),
        out_shape=jax.ShapeDtypeStruct((rows // 2, weight.shape[1]), f32),
        in_specs=[VMEM] * (len(parts) + 1) + [ANY] * len(after),
        out_specs=VMEM,
        compiler_params=pltpu.CompilerParams(vmem_limit_bytes=8 * MIB),
        cost_estimate=pl.CostEstimate(flops=10**8, bytes_accessed=2 * MIB, transcendentals=0),
        name="project",
    )(*parts, weight, *after)


def tower_kernel(block, features_ref, w1_ref, w2_ref, after_ref, high_ref, low_ref):
    for start in range(0, features_ref.shape[0], block):
        at = pl.ds(start, block)
        hidden = jnp.dot(features_ref[at, :], w1_ref[...], preferred_element_type=f32)
        hidden = 0.5 * hidden * (1.0 + lax.erf(hidden * (0.5**0.5)))
        emb = jnp.dot(hidden.astype(bf16), w2_ref[...], preferred_element_type=f32)
        emb = emb * lax.rsqrt(jnp.mean(emb * emb, axis=1, keepdims=True) + epsilon)
        high = emb.astype(bf16)
        high_ref[at, :] = high
        low_ref[at, :] = (emb - high.astype(f32)).astype(bf16)


def tower(part, parts, features, w1, w2, after):
    users = features.shape[0] // parts
    embed = w2.shape[1]
    whole = lambda i: (0, 0)
    shape = jax.ShapeDtypeStruct((users, embed), bf16)
    return pl.pallas_call(
        functools.partial(tower_kernel, min(256, users)),
        grid=(1,),
        out_shape=(shape, shape),
        in_specs=[
            pl.BlockSpec((users, features.shape[1]), lambda i: (part, 0)),
            VMEM,
            VMEM,
            ANY,
        ],
        out_specs=(pl.BlockSpec((users, embed), whole), pl.BlockSpec((users, embed), whole)),
        compiler_params=pltpu.CompilerParams(vmem_limit_bytes=16 * MIB),
        cost_estimate=pl.CostEstimate(
            flops=2 * users * (w1.size + w2.size), bytes_accessed=2 * MIB, transcendentals=users * w1.shape[1]
        ),
    )(features, w1, w2, after)


def split(x, size):
    if size & (size - 1) == 0:
        return x >> (size.bit_length() - 1), x & (size - 1)
    return lax.div(x, jnp.full_like(x, size)), lax.rem(x, jnp.full_like(x, size))


def unit_rows(rows):
    return rows * lax.rsqrt(jnp.mean(rows * rows, axis=1, keepdims=True) + epsilon)


def scores_kernel(count, block, own, other, positive_ref, mine_ref, *refs):
    t, c, d = (lax.axis_index(axis) for axis in ("tab", "cand", "dp"))
    C, D = lax.axis_size("cand"), lax.axis_size("dp")
    half = mine_ref.shape[0]
    first = lax.rem(d + other, 2) * half
    emb = unit_rows(mine_ref[...])
    items = emb * (logit_scale / emb.shape[1] * log2_e)
    item_high = items.astype(bf16)
    item_low = (items - item_high.astype(f32)).astype(bf16)
    users = refs[0].shape[0]
    out_ref = refs[-1]
    if other:
        before_ref, earlier_ref, item_ref, out_ref, emb_ref = refs[-5:]
        emb_ref[pl.ds(0, half), :] = emb
        emb_ref[pl.ds(half, half), :] = unit_rows(earlier_ref[...])

    def dot(a, b):
        return lax.dot_general(a, b, (((1,), (1,)), ((), ())), preferred_element_type=f32)

    for k in range(count):
        high_ref, low_ref = refs[2 * k], refs[2 * k + 1]
        for start in range(0, users, block):
            at = pl.ds(start, block)
            high = high_ref[at, :]
            scores = dot(item_high, high) + (dot(item_low, high) + dot(item_high, low_ref[at, :]))
            to = pl.ds(k * users + start, block)
            rest, within = split(positive_ref[:, to], own)
            rest, owner_d = split(rest, D)
            owner_t, owner_c = split(rest, C)
            place = (owner_t * D + owner_d) * own + within - first
            place = jnp.where(owner_c == c, place, -1)
            here = lax.broadcasted_iota(jnp.int32, scores.shape, 0) == place
            total = jnp.sum(jnp.exp2(scores), axis=0, keepdims=True)
            positive = jnp.sum(jnp.where(here, scores, 0.0), axis=0, keepdims=True)
            if other:
                total = total + before_ref[pl.ds(0, 1), to]
                positive = positive + before_ref[pl.ds(1, 1), to]
            out_ref[pl.ds(0, 1), to] = total
            out_ref[pl.ds(1, 1), to] = positive
    if other:
        row = (t * D + d) * own - first
        row = jnp.where(row < 0, row + 2 * half, row)
        step = 8 if own % 8 == 0 else 1
        for k in range(0, own, step):
            item_ref[pl.ds(k, step), :] = emb_ref[pl.ds(pl.multiple_of(row + k, step), step), :]


def score(positives, rows, embs, own, earlier=()):
    count = len(embs)
    users = embs[0][0].shape[0]
    flat = [x for pair in embs for x in pair] + list(earlier)
    total = users * count
    other = len(earlier) // 2
    item = (jax.ShapeDtypeStruct((own, rows.shape[1]), f32),) * other
    return pl.pallas_call(
        functools.partial(scores_kernel, count, min(512, users), own, other),
        out_shape=item + (jax.ShapeDtypeStruct((2, total), f32),),
        in_specs=[VMEM] * (2 + len(flat)),
        out_specs=(VMEM,) * (1 + other),
        scratch_shapes=[pltpu.VMEM((2 * rows.shape[0], rows.shape[1]), f32)] * other,
        compiler_params=pltpu.CompilerParams(vmem_limit_bytes=16 * MIB),
        cost_estimate=pl.CostEstimate(
            flops=6 * total * rows.shape[1] * rows.shape[0], bytes_accessed=2 * MIB, transcendentals=0
        ),
    )(positives, rows, *flat)


def finish_kernel(*refs):
    total = refs[0][...]
    for ref in refs[1:-1]:
        total = total + ref[...]
    refs[-1][...] = (jnp.log2(total[:1]) - total[1:]) * ln_2


def finish(partials):
    return pl.pallas_call(
        finish_kernel,
        out_shape=jax.ShapeDtypeStruct((1, partials[0].shape[1]), f32),
        in_specs=[VMEM] * len(partials),
        out_specs=VMEM,
        compiler_params=pltpu.CompilerParams(vmem_limit_bytes=4 * MIB),
        name="finish",
    )(*partials).reshape(-1)


def swap(x, axis, bit):
    return lax.ppermute(x, axis, [(i, i ^ bit) for i in range(lax.axis_size(axis))])


def swap_both(x, bit_dp, bit_tab):
    T, D = lax.axis_size("tab"), lax.axis_size("dp")
    pairs = [(t * D + d, (t ^ bit_tab) * D + (d ^ bit_dp)) for t in range(T) for d in range(D)]
    return lax.ppermute(x, ("tab", "dp"), pairs)


def shift(x, axis, by):
    size = lax.axis_size(axis)
    return lax.ppermute(x, axis, [(i, (i + by) % size) for i in range(size)])


def bits_of(axis):
    return [(axis, 1 << k) for k in range(lax.axis_size(axis).bit_length() - 1)]


def body(
    tables, bag_ids, bag_lengths, item_weight, user_features, user_w1, user_w2, positive_items
):
    table = tables[0]
    ids = bag_ids[0].T
    T, C, D = lax.axis_size("tab"), lax.axis_size("cand"), lax.axis_size("dp")
    positions, items = ids.shape
    own = items // (T * C * D)
    count = items // C

    wide = widen(table)
    places, inverse = place(ids, bag_lengths, wide, T, C)
    order = pool_order(C)
    after = places
    received = []
    for j in order:
        part = pool(j, inverse, wide, places, after, count, positions, items // (T * C))
        after = part
        if j:
            part = shift(part, "cand", j)
        received.append(part)

    send = project(order, 1, received, item_weight, ())
    came = swap(send, "dp", 1)
    keep = project(order, 0, received, item_weight, (send,))
    total = keep + came
    embs = []
    for k in range(tower_parts):
        embs.append(tower(k, tower_parts, user_features, user_w1, user_w2, send))
    steps = [step for step in bits_of("dp") if step[1] > 1] + bits_of("tab")
    if len(steps) == 2:
        moved = []
        for picked in ((1, 1), (1, 0), (0, 1)):
            moved.append(swap_both(total, picked[0] * steps[0][1], picked[1] * steps[1][1]))
        total = (total + moved[1]) + (moved[2] + moved[0])
    else:
        for step in steps:
            total = total + swap(total, *step)
    positives = positive_items[None]
    other = swap(total, "dp", 1)
    (partial,) = score(positives, total, embs, own)
    item_emb, partial = score(positives, other, embs, own, (partial, total))
    partials = [partial]
    for j in range(1, C):
        partials.append(swap(partial, "cand", j))
    return (item_emb, finish(partials))


def pool_order(C):
    return tuple(range(C - 1, -1, -1))


def solution(mesh):
    placed = (
        P(("cand", "dp"), "tab", None),
        P(("cand", "dp"), None, None),
        P(("cand", "dp"), None),
        P(),
        P(("tab", "dp"), None),
        P(),
        P(),
        P(("tab", "dp")),
    )
    return jax.shard_map(
        body,
        mesh=mesh,
        in_specs=placed,
        out_specs=(P(("tab", "cand", "dp"), None), P(("tab", "dp"))),
        check_vma=False,
    )
```

```python
import functools

import jax
import jax.numpy as jnp
from jax import lax
from jax.experimental import pallas as pl
from jax.experimental.pallas import tpu as pltpu
from jax.sharding import PartitionSpec as P


epsilon = 1e-06
logit_scale = 20.0
log2_e = 1.4426950408889634
ln_2 = 0.6931471805599453


f32 = jnp.float32
bf16 = jnp.bfloat16
VMEM = pl.BlockSpec(memory_space=pltpu.VMEM)
SMEM = pl.BlockSpec(memory_space=pltpu.SMEM)
ANY = pl.BlockSpec(memory_space=pl.ANY)
MIB = 1 << 20
zero_rows = 8
bags_at_once = 32
tower_parts = 2


def table_copies(table_ref, raw, sems):
    pieces = sems.shape[0]
    piece = table_ref.shape[0] // pieces
    return [
        pltpu.make_async_copy(
            table_ref.at[pl.ds(k * piece, piece)], raw.at[pl.ds(k * piece, piece)], sems.at[k]
        )
        for k in range(pieces)
    ]


def widen_into(copies, first, last, raw, wide_ref):
    rows = raw.shape[0]
    piece = rows // len(copies)
    block = min(1024, piece)
    if first == 0:
        wide_ref[pl.ds(rows, zero_rows), :] = jnp.zeros((zero_rows, wide_ref.shape[1]), f32)
    for k in range(first, last):
        copies[k].wait()

        @pl.loop(0, piece // block)
        def _(i):
            at = pl.ds(pl.multiple_of(k * piece + i * block, block), block)
            wide_ref[at, :] = raw[at, :].astype(f32)


def widen_kernel(table_ref, wide_ref, raw, sems):
    copies = table_copies(table_ref, raw, sems)
    for copy in copies:
        copy.start()
    widen_into(copies, 0, len(copies), raw, wide_ref)


def widen(table):
    rows, width = table.shape
    pieces = 8
    return pl.pallas_call(
        widen_kernel,
        out_shape=pltpu.VMEM((rows + zero_rows, width), f32),
        in_specs=[pl.BlockSpec(memory_space=pltpu.HBM)],
        out_specs=VMEM,
        scratch_shapes=[pltpu.VMEM((rows, width), bf16), pltpu.SemaphoreType.DMA((pieces,))],
        compiler_params=pltpu.CompilerParams(vmem_limit_bytes=30 * MIB),
        cost_estimate=pl.CostEstimate(flops=10**6, bytes_accessed=rows * width * 2, transcendentals=0),
        name="widen",
    )(table)


def place_into(T, C, rows, ids, lengths, places_ref, inverse_ref):
    positions, items = ids.shape
    run = items // (T * C)
    local = ids - lax.axis_index("tab") * rows
    valid = lax.broadcasted_iota(jnp.int32, local.shape, 0) < lengths
    places = jnp.where((local >= 0) & (local < rows) & valid, local, rows)
    inverse = 1.0 / lengths.astype(f32)
    for t in range(T):
        for c in range(C):
            at = (t * C + c) * run
            to = pl.ds((c * T + t) * positions, positions)
            places_ref[to, :] = places[:, at : at + run]
            inverse_ref[pl.ds(c * T + t, 1), :] = inverse[:, at : at + run]


def pool_run(positions, run, t, wide_ref, places, inverse, first, out_ref):
    at_once = min(bags_at_once, run)
    index_refs = [places.at[pl.ds((t * positions + p) * run, run)] for p in range(positions)]

    @pl.loop(0, run // at_once)
    def _(b):
        for u in range(at_once):
            i = b * at_once + u
            rows = [wide_ref[pl.ds(ref[i], 1), :] for ref in index_refs]
            while len(rows) > 1:
                rows = [sum(rows[n : n + 2][1:], rows[n]) for n in range(0, len(rows), 2)]
            out_ref[pl.ds(t * run + i, 1), :] = rows[0] * inverse[first + i]


def chunk_of(ahead):
    return lax.rem(lax.axis_index("cand") + ahead, lax.axis_size("cand"))


def widen_pool_kernel(T, C, ahead, table_ref, ids_ref, lengths_ref, *refs):
    wide_ref, places_ref, inverse_ref, out_ref = refs[:4]
    raw, ids, lengths, rows_i, rows_f, near_i, near_f, table_sems, bag_sems, sems = refs[4:]
    positions = ids.shape[0]
    run = out_ref.shape[0] // T
    copies = table_copies(table_ref, raw, table_sems)
    bags = [
        pltpu.make_async_copy(ids_ref, ids, bag_sems.at[0]),
        pltpu.make_async_copy(lengths_ref, lengths, bag_sems.at[1]),
    ]
    for copy in copies[:2] + bags + copies[2:]:
        copy.start()
    middle = len(copies) // 2
    widen_into(copies, 0, middle, raw, wide_ref)
    for copy in bags:
        copy.wait()
    place_into(T, C, table_ref.shape[0], ids[...], lengths[...], places_ref, inverse_ref)
    chunk = chunk_of(ahead)
    nears = []
    for t in range(T):
        rows_f[t] = inverse_ref[pl.ds(chunk * T + t, 1), :]
        nears.append((rows_f.at[t, 0], near_f.at[pl.ds(t * run, run)]))
        for p in range(positions):
            k = t * positions + p
            rows_i[k] = places_ref[pl.ds(chunk * (T * positions) + k, 1), :]
            nears.append((rows_i.at[k, 0], near_i.at[pl.ds(k * run, run)]))
    nears = [pltpu.make_async_copy(a, b, sems.at[k]) for k, (a, b) in enumerate(nears)]
    for copy in nears:
        copy.start()
    widen_into(copies, middle, len(copies), raw, wide_ref)
    for copy in nears:
        copy.wait()
    for t in range(T):
        pool_run(positions, run, t, wide_ref, near_i, near_f, t * run, out_ref)


def widen_pool(table, ids, lengths, T, C, ahead):
    rows, width = table.shape
    positions, items = ids.shape
    run = items // (T * C)
    pieces = 8
    hbm = pl.BlockSpec(memory_space=pltpu.HBM)
    in_hbm = lambda x: pltpu.with_memory_space_constraint(x, pltpu.HBM)
    wide, places, inverse, out = pl.pallas_call(
        functools.partial(widen_pool_kernel, T, C, ahead),
        out_shape=(
            pltpu.VMEM((rows + zero_rows, width), f32),
            jax.ShapeDtypeStruct((C * T * positions, run), jnp.int32),
            jax.ShapeDtypeStruct((C * T, run), f32),
            jax.ShapeDtypeStruct((items // C, width), f32),
        ),
        in_specs=[hbm, hbm, hbm],
        out_specs=(VMEM,) * 4,
        scratch_shapes=[
            pltpu.VMEM((rows, width), bf16),
            pltpu.VMEM(ids.shape, jnp.int32),
            pltpu.VMEM(lengths.shape, jnp.int32),
            pltpu.VMEM((T * positions, 1, run), jnp.int32),
            pltpu.VMEM((T, 1, run), f32),
            pltpu.SMEM((T * positions * run,), jnp.int32),
            pltpu.SMEM((T * run,), f32),
            pltpu.SemaphoreType.DMA((pieces,)),
            pltpu.SemaphoreType.DMA((2,)),
            pltpu.SemaphoreType.DMA((T * (positions + 1),)),
        ],
        compiler_params=pltpu.CompilerParams(vmem_limit_bytes=30 * MIB),
        cost_estimate=pl.CostEstimate(flops=10**7, bytes_accessed=rows * width * 2, transcendentals=0),
        name="widen_pool",
    )(table, in_hbm(ids), in_hbm(lengths))
    return wide, places.reshape(-1), inverse.reshape(-1), out


def place(ids, lengths, rows, T, C):
    positions, items = ids.shape
    run = items // (T * C)
    local = ids - lax.axis_index("tab") * rows
    valid = lax.broadcasted_iota(jnp.int32, ids.shape, 0) < lengths
    places = jnp.where((local >= 0) & (local < rows) & valid, local, rows)
    places = places.reshape(positions, T, C, run).transpose(2, 1, 0, 3).reshape(-1)
    inverse = (1.0 / lengths.astype(f32)).reshape(T, C, run).transpose(1, 0, 2).reshape(-1)
    return places, inverse


def pool_kernel(positions, run, ahead, inverse_ref, wide_ref, places_ref, after_ref, out_ref, *refs):
    places, inverse, sems = refs
    count = out_ref.shape[0]
    size = count * positions
    pieces = sems.shape[0] - 1
    chunk = chunk_of(ahead)
    copies = [pltpu.make_async_copy(inverse_ref, inverse, sems.at[pieces])]
    for k in range(pieces):
        piece = size // pieces
        start = pl.multiple_of(chunk * size + k * piece, piece)
        copies.append(
            pltpu.make_async_copy(
                places_ref.at[pl.ds(start, piece)], places.at[pl.ds(k * piece, piece)], sems.at[k]
            )
        )
    for copy in copies:
        copy.start()
    copies[0].wait()
    for t in range(count // run):
        if t < pieces:
            copies[t + 1].wait()
        pool_run(positions, run, t, wide_ref, places, inverse, chunk * count + t * run, out_ref)


def pool(ahead, inverse, wide, places, after, count, positions, run):
    width = wide.shape[1]
    pieces = count // run if positions * run % 1024 == 0 else 1
    return pl.pallas_call(
        functools.partial(pool_kernel, positions, run, ahead),
        out_shape=jax.ShapeDtypeStruct((count, width), f32),
        in_specs=[ANY, VMEM, ANY, ANY],
        out_specs=VMEM,
        scratch_shapes=[
            pltpu.SMEM((count * positions,), jnp.int32),
            pltpu.SMEM(inverse.shape, f32),
            pltpu.SemaphoreType.DMA((pieces + 1,)),
        ],
        compiler_params=pltpu.CompilerParams(vmem_limit_bytes=20 * MIB),
        cost_estimate=pl.CostEstimate(
            flops=10**7, bytes_accessed=count * width * 4, transcendentals=0
        ),
        name="pool",
    )(inverse, wide, places, after)


def project_kernel(order, other, *refs):
    count = len(order)
    parts, weight_ref, out_ref = refs[:count], refs[count], refs[-1]
    half = out_ref.shape[0]
    width = parts[0].shape[1]
    c, d = lax.axis_index("cand"), lax.axis_index("dp")
    C, D = lax.axis_size("cand"), lax.axis_size("dp")
    which = lax.rem(d + other, 2)
    at = pl.ds(pl.multiple_of(which * half, half), half)
    total = None
    for k in range(count):
        value = parts[k][at, :]
        source = lax.rem(c + C - order[k], C) * D + d
        weight = weight_ref[pl.ds(pl.multiple_of(source * width, width), width), :]
        for _ in range(3):
            short = value.astype(bf16)
            term = jnp.dot(short, weight, preferred_element_type=f32)
            total = term if total is None else total + term
            value = value - short.astype(f32)
    out_ref[...] = total


def project(order, other, parts, weight, after):
    rows = parts[0].shape[0]
    return pl.pallas_call(
        functools.partial(project_kernel, order, other),
        out_shape=jax.ShapeDtypeStruct((rows // 2, weight.shape[1]), f32),
        in_specs=[VMEM] * (len(parts) + 1) + [ANY] * len(after),
        out_specs=VMEM,
        compiler_params=pltpu.CompilerParams(vmem_limit_bytes=8 * MIB),
        cost_estimate=pl.CostEstimate(flops=10**8, bytes_accessed=2 * MIB, transcendentals=0),
        name="project",
    )(*parts, weight, *after)


def tower_kernel(block, features_ref, w1_ref, w2_ref, after_ref, high_ref, low_ref):
    for start in range(0, features_ref.shape[0], block):
        at = pl.ds(start, block)
        hidden = jnp.dot(features_ref[at, :], w1_ref[...], preferred_element_type=f32)
        hidden = 0.5 * hidden * (1.0 + lax.erf(hidden * (0.5**0.5)))
        emb = jnp.dot(hidden.astype(bf16), w2_ref[...], preferred_element_type=f32)
        emb = emb * lax.rsqrt(jnp.mean(emb * emb, axis=1, keepdims=True) + epsilon)
        high = emb.astype(bf16)
        high_ref[at, :] = high
        low_ref[at, :] = (emb - high.astype(f32)).astype(bf16)


def tower(part, parts, features, w1, w2, after):
    users = features.shape[0] // parts
    embed = w2.shape[1]
    whole = lambda i: (0, 0)
    shape = jax.ShapeDtypeStruct((users, embed), bf16)
    return pl.pallas_call(
        functools.partial(tower_kernel, min(256, users)),
        grid=(1,),
        out_shape=(shape, shape),
        in_specs=[
            pl.BlockSpec((users, features.shape[1]), lambda i: (part, 0)),
            VMEM,
            VMEM,
            ANY,
        ],
        out_specs=(pl.BlockSpec((users, embed), whole), pl.BlockSpec((users, embed), whole)),
        compiler_params=pltpu.CompilerParams(vmem_limit_bytes=16 * MIB),
        cost_estimate=pl.CostEstimate(
            flops=2 * users * (w1.size + w2.size), bytes_accessed=2 * MIB, transcendentals=users * w1.shape[1]
        ),
    )(features, w1, w2, after)


def split(x, size):
    if size & (size - 1) == 0:
        return x >> (size.bit_length() - 1), x & (size - 1)
    return lax.div(x, jnp.full_like(x, size)), lax.rem(x, jnp.full_like(x, size))


def unit_rows(rows):
    return rows * lax.rsqrt(jnp.mean(rows * rows, axis=1, keepdims=True) + epsilon)


def scores_kernel(count, block, own, other, positive_ref, mine_ref, *refs):
    t, c, d = (lax.axis_index(axis) for axis in ("tab", "cand", "dp"))
    C, D = lax.axis_size("cand"), lax.axis_size("dp")
    half = mine_ref.shape[0]
    first = lax.rem(d + other, 2) * half
    emb = unit_rows(mine_ref[...])
    items = emb * (logit_scale / emb.shape[1] * log2_e)
    item_high = items.astype(bf16)
    item_low = (items - item_high.astype(f32)).astype(bf16)
    users = refs[0].shape[0]
    out_ref = refs[-1]
    if other:
        before_ref, earlier_ref, item_ref, out_ref, emb_ref = refs[-5:]
        emb_ref[pl.ds(0, half), :] = emb
        emb_ref[pl.ds(half, half), :] = unit_rows(earlier_ref[...])

    def dot(a, b):
        return lax.dot_general(a, b, (((1,), (1,)), ((), ())), preferred_element_type=f32)

    for k in range(count):
        high_ref, low_ref = refs[2 * k], refs[2 * k + 1]
        for start in range(0, users, block):
            at = pl.ds(start, block)
            high = high_ref[at, :]
            scores = dot(item_high, high) + (dot(item_low, high) + dot(item_high, low_ref[at, :]))
            to = pl.ds(k * users + start, block)
            rest, within = split(positive_ref[:, to], own)
            rest, owner_d = split(rest, D)
            owner_t, owner_c = split(rest, C)
            place = (owner_t * D + owner_d) * own + within - first
            place = jnp.where(owner_c == c, place, -1)
            here = lax.broadcasted_iota(jnp.int32, scores.shape, 0) == place
            total = jnp.sum(jnp.exp2(scores), axis=0, keepdims=True)
            positive = jnp.sum(jnp.where(here, scores, 0.0), axis=0, keepdims=True)
            if other:
                total = total + before_ref[pl.ds(0, 1), to]
                positive = positive + before_ref[pl.ds(1, 1), to]
            out_ref[pl.ds(0, 1), to] = total
            out_ref[pl.ds(1, 1), to] = positive
    if other:
        row = (t * D + d) * own - first
        row = jnp.where(row < 0, row + 2 * half, row)
        step = 8 if own % 8 == 0 else 1
        for k in range(0, own, step):
            item_ref[pl.ds(k, step), :] = emb_ref[pl.ds(pl.multiple_of(row + k, step), step), :]


def score(positives, rows, embs, own, earlier=()):
    count = len(embs)
    users = embs[0][0].shape[0]
    flat = [x for pair in embs for x in pair] + list(earlier)
    total = users * count
    other = len(earlier) // 2
    item = (jax.ShapeDtypeStruct((own, rows.shape[1]), f32),) * other
    return pl.pallas_call(
        functools.partial(scores_kernel, count, min(1024, users), own, other),
        out_shape=item + (jax.ShapeDtypeStruct((2, total), f32),),
        in_specs=[VMEM] * (2 + len(flat)),
        out_specs=(VMEM,) * (1 + other),
        scratch_shapes=[pltpu.VMEM((2 * rows.shape[0], rows.shape[1]), f32)] * other,
        compiler_params=pltpu.CompilerParams(vmem_limit_bytes=16 * MIB),
        cost_estimate=pl.CostEstimate(
            flops=6 * total * rows.shape[1] * rows.shape[0], bytes_accessed=2 * MIB, transcendentals=0
        ),
    )(positives, rows, *flat)


def finish_kernel(*refs):
    total = refs[0][...]
    for ref in refs[1:-1]:
        total = total + ref[...]
    refs[-1][...] = (jnp.log2(total[:1]) - total[1:]) * ln_2


def finish(partials):
    return pl.pallas_call(
        finish_kernel,
        out_shape=jax.ShapeDtypeStruct((1, partials[0].shape[1]), f32),
        in_specs=[VMEM] * len(partials),
        out_specs=VMEM,
        compiler_params=pltpu.CompilerParams(vmem_limit_bytes=4 * MIB),
        name="finish",
    )(*partials).reshape(-1)


def swap(x, axis, bit):
    return lax.ppermute(x, axis, [(i, i ^ bit) for i in range(lax.axis_size(axis))])


def swap_both(x, bit_dp, bit_tab):
    T, D = lax.axis_size("tab"), lax.axis_size("dp")
    pairs = [(t * D + d, (t ^ bit_tab) * D + (d ^ bit_dp)) for t in range(T) for d in range(D)]
    return lax.ppermute(x, ("tab", "dp"), pairs)


def shift(x, axis, by):
    size = lax.axis_size(axis)
    return lax.ppermute(x, axis, [(i, (i + by) % size) for i in range(size)])


def bits_of(axis):
    return [(axis, 1 << k) for k in range(lax.axis_size(axis).bit_length() - 1)]


def body(
    tables, bag_ids, bag_lengths, item_weight, user_features, user_w1, user_w2, positive_items
):
    table = tables[0]
    ids = bag_ids[0].T
    T, C, D = lax.axis_size("tab"), lax.axis_size("cand"), lax.axis_size("dp")
    positions, items = ids.shape
    own = items // (T * C * D)
    count = items // C

    order = pool_order(C)
    run = items // (T * C)
    first = None
    if run % 128 == 0:
        wide, places, inverse, first = widen_pool(table, ids, bag_lengths, T, C, order[0])
    else:
        wide = widen(table)
        places, inverse = place(ids, bag_lengths, table.shape[0], T, C)
    after = places
    received = []
    for k, j in enumerate(order):
        part = first
        if k or first is None:
            part = pool(j, inverse, wide, places, after, count, positions, run)
        after = part
        if j:
            part = shift(part, "cand", j)
        received.append(part)

    send = project(order, 1, received, item_weight, ())
    came = swap(send, "dp", 1)
    keep = project(order, 0, received, item_weight, (send,))
    total = keep + came
    embs = []
    for k in range(tower_parts):
        embs.append(tower(k, tower_parts, user_features, user_w1, user_w2, send))
    steps = [step for step in bits_of("dp") if step[1] > 1] + bits_of("tab")
    if len(steps) == 2:
        moved = []
        for picked in ((1, 1), (1, 0), (0, 1)):
            moved.append(swap_both(total, picked[0] * steps[0][1], picked[1] * steps[1][1]))
        total = (total + moved[1]) + (moved[2] + moved[0])
    else:
        for step in steps:
            total = total + swap(total, *step)
    positives = positive_items[None]
    other = swap(total, "dp", 1)
    (partial,) = score(positives, total, embs, own)
    item_emb, partial = score(positives, other, embs, own, (partial, total))
    partials = [partial]
    for j in range(1, C):
        partials.append(swap(partial, "cand", j))
    return (item_emb, finish(partials))


def pool_order(C):
    return tuple(range(C - 1, -1, -1))


def solution(mesh):
    placed = (
        P(("cand", "dp"), "tab", None),
        P(("cand", "dp"), None, None),
        P(("cand", "dp"), None),
        P(),
        P(("tab", "dp"), None),
        P(),
        P(),
        P(("tab", "dp")),
    )
    return jax.shard_map(
        body,
        mesh=mesh,
        in_specs=placed,
        out_specs=(P(("tab", "cand", "dp"), None), P(("tab", "dp"))),
        check_vma=False,
    )
```
